32 devices in a mesh: map: 8 (over z, y), rep: 4 (over x, core).
Axes of the slice: x: 2, y: 2, z: 4, core: 2. Of those that a mesh axis runs over, the one named last changes fastest.
Arguments:
- field_bricks: bfloat16 [16384, 512], P('map'), may hold values from -6 to 6
- owners: int32 [2048, 64], P('map', 'rep'), may hold values from 0 to 7, as said below
- bricks: int32 [2048, 64], P('map', 'rep'), may hold values from 0 to 2047
- corners: int32 [2048, 64], P('map', 'rep'), may hold values from 0 to 342
- fraction: float32 [3, 2048, 64], P(None, 'map', 'rep'), may hold values from 0 to 1
Outputs:
- trajectory_cost: float32 [2048], P('map')
- waypoint_grad: float32 [3, 2048, 64], P(None, 'map', 'rep')
The draws below stay inside these ranges and needn't reach their ends.
Inputs may be any that keep to these rules, and one draw needn't show every extreme that they name: `owners`: among one device's 4096 waypoints at most 2048 have the same owner, and in every draw some owner has exactly 2048 of them.
All inputs are finite; a program needn't handle non-finite values.
Results may differ from the reference program's by a relative error of at most 0.0003.
Values sent between devices are 32-bit elements; how exact they have to be, the bound alone decides.
A program may use at most 64 MiB of HBM per device.

```python
import jax
import jax.numpy as jnp

VOXELS = 512
WAYPOINTS = 64
BRICK_DEV = 2048
TRAJ_DEV = 256
BRICKS = 16384
TRAJECTORIES = 2048
N_MAP = 8
N_REP = 4


def draw_owners(key, part):
    per_device = TRAJ_DEV * WAYPOINTS // N_REP
    capacity = 4 * per_device // N_MAP
    remaining = per_device - capacity - capacity // 2
    even_share = remaining // (N_MAP - 2)
    leftover = remaining % (N_MAP - 2)
    places = jnp.arange(N_MAP, dtype=jnp.int32)
    quota = jnp.where(places == 0, capacity, jnp.where(places == 1, capacity // 2, even_share + (places - 2 < leftover).astype(jnp.int32)))
    limits = jnp.cumsum(quota)
    positions = jnp.arange(per_device, dtype=jnp.int32)
    which = jnp.sum((limits[None, :] <= positions[:, None]).astype(jnp.int32), axis=1)

    def one_block(block_key):
        first_key, second_key = jax.random.split(block_key)
        labels = jax.random.permutation(first_key, places)
        return jax.random.permutation(second_key, labels[which])
    block_keys = jax.random.split(jax.random.fold_in(key, 17), N_MAP * N_REP)
    blocks = jax.vmap(one_block)(block_keys).reshape(N_MAP, N_REP, TRAJ_DEV, WAYPOINTS // N_REP)
    return blocks.transpose(0, 2, 1, 3).reshape(N_MAP * TRAJ_DEV, WAYPOINTS).astype(jnp.int32)


def place_ends(result, own_key, least, top_value):
    longest = result.shape.index(max(result.shape))
    spots = []
    for shift in (0, 1):
        where = [jax.random.randint(jax.random.fold_in(own_key, axis), (), 0, length) for axis, length in enumerate(result.shape)]
        where[longest] = (where[longest] + shift) % result.shape[longest]
        spots.append(tuple(where))
    return result.at[spots[0]].set(least).at[spots[1]].set(top_value)


def steps_of(rng, shape, cuts, smallest, top_value):
    def one(position, shards_of):
        heights = jax.random.uniform(jax.random.fold_in(jax.random.fold_in(rng, 6), position), (shards_of,), jnp.float32, smallest / len(cuts), top_value / len(cuts))
        return jnp.repeat(jnp.exp(heights), shape[position] // shards_of).reshape((-1,) + (1,) * (len(shape) - position - 1))

    level = one(*cuts[0])
    for cut in cuts[1:]:
        level = level * one(*cut)
    return level


def normal_values(key, extent, deviation, reach, pieces=(), kind=jnp.bfloat16):
    values = jax.random.normal(key, extent, jnp.float32) * deviation
    if len(pieces) > 0:
        values = steps_of(key, extent, pieces, -0.22, 0.18) * values
    return jnp.clip(values, min=-reach, max=reach).astype(kind)


def setup_inputs(seed: int = 0) -> dict:
    seeds = jax.random.split(jax.random.key(seed), 6)
    field_bricks = normal_values(seeds[0], (BRICKS, VOXELS), 1.0, 6.0, ((0, 8),))
    owners = draw_owners(jax.random.fold_in(seeds[5], 71), 0)
    bricks = place_ends(jax.random.randint(seeds[2], (TRAJECTORIES, WAYPOINTS), 0, BRICK_DEV), jax.random.fold_in(seeds[2], 1), 0, BRICK_DEV - 1).astype(jnp.int32)
    corners = place_ends(jax.random.randint(seeds[3], (TRAJECTORIES, WAYPOINTS), 0, 343), jax.random.fold_in(seeds[3], 1), 0, 342).astype(jnp.int32)
    fraction = jnp.clip(1.0 * jax.random.uniform(seeds[4], (3, TRAJECTORIES, WAYPOINTS), jnp.float32) ** steps_of(seeds[4], (3, TRAJECTORIES, WAYPOINTS), ((1, 8), (2, 4)), -0.2, 0.2), 0.0, 1.0)
    return dict(field_bricks=field_bricks, owners=owners, bricks=bricks, corners=corners, fraction=fraction)


margin = 0.5


def corner_offset(corners):
    return (corners // 49) * 64 + ((corners // 7) % 7) * 8 + corners % 7


def lookup(slab_flat, cell_code, frac_x, frac_y, frac_z, stack_axis):
    total = jnp.zeros(frac_x.shape, jnp.float32)
    slope_x = jnp.zeros(frac_x.shape, jnp.float32)
    slope_y = jnp.zeros(frac_x.shape, jnp.float32)
    slope_z = jnp.zeros(frac_x.shape, jnp.float32)
    for step_x in (0, 1):
        weight_x = frac_x if step_x else 1.0 - frac_x
        sign_x = 1.0 if step_x else -1.0
        for step_y in (0, 1):
            weight_y = frac_y if step_y else 1.0 - frac_y
            sign_y = 1.0 if step_y else -1.0
            for step_z in (0, 1):
                weight_z = frac_z if step_z else 1.0 - frac_z
                sign_z = 1.0 if step_z else -1.0
                value = slab_flat[cell_code + (step_x * 64 + step_y * 8 + step_z)].astype(jnp.float32)
                total = total + weight_x * weight_y * weight_z * value
                slope_x = slope_x + sign_x * weight_y * weight_z * value
                slope_y = slope_y + sign_y * weight_x * weight_z * value
                slope_z = slope_z + sign_z * weight_x * weight_y * value
    return jnp.stack([total, slope_x, slope_y, slope_z], axis=stack_axis)


def reference(field_bricks, owners, bricks, corners, fraction):
    slab_flat = field_bricks.reshape(-1)
    cell_code = ((owners * BRICK_DEV + bricks) * 512 + corner_offset(corners)).astype(jnp.int32)
    answers = lookup(slab_flat, cell_code, fraction[0], fraction[1], fraction[2], 0)
    hinge_term = jnp.maximum(margin - answers[0], 0.0)
    trajectory_cost = jnp.sum(hinge_term * hinge_term, axis=1)
    waypoint_grad = -2.0 * hinge_term[None] * answers[1:]
    return trajectory_cost, waypoint_grad
```

```python
import functools

import jax
import jax.numpy as jnp
from jax import lax
from jax.experimental import pallas as pl
from jax.experimental.pallas import tpu as pltpu
from jax.sharding import PartitionSpec as P

margin = 0.5
LANES = 128
VMEM = pltpu.VMEM
SMEM = pltpu.SMEM


def lanes_of(x):
    xt = x.T
    return jnp.concatenate(
        [xt[:, h * LANES : (h + 1) * LANES] for h in range(x.shape[0] // LANES)], axis=0
    )


def iota(shape, axis):
    return lax.broadcasted_iota(jnp.int32, shape, axis)


def each(count, body, unrolled):
    if count <= unrolled:
        for i in range(count):
            body(i)
    else:
        lax.fori_loop(0, count, lambda i, z: (body(i), z)[1], 0)


def dispatch_kernel(
    devices, tiles, owners_ref, bricks_ref, corners_ref, frac_ref,
    out_ref, own_ref, rank_ref, meta_ref,
    data_ref, pos_ref, meta_s, sem,
):
    own = lanes_of(owners_ref[...].astype(jnp.float32)).astype(jnp.int32)
    chunks = own.shape[0]
    bricks = bricks_ref[...]
    corners = corners_ref[...]
    cx = (corners * 1338) >> 16
    cxy = (corners * 9363) >> 16
    code = bricks * 512 + cx * 64 + (cxy - cx * 7) * 8 + (corners - cxy * 7)
    code = lanes_of(code.astype(jnp.float32))
    for k in range(2):
        data_ref[:, 4 * k, :] = code
    for f in range(3):
        part = lanes_of(frac_ref[f])
        for k in range(2):
            data_ref[:, 4 * k + 1 + f, :] = part
    own_ref[...] = own
    out_ref[...] = jnp.zeros_like(out_ref)

    upper = (iota((LANES, LANES), 0) <= iota((LANES, LANES), 1)).astype(jnp.float32).astype(jnp.bfloat16)
    ones = jnp.ones((LANES, LANES), jnp.bfloat16)
    before = (iota((chunks, chunks), 0) > iota((chunks, chunks), 1)).astype(jnp.float32).astype(jnp.bfloat16)
    lane = iota((chunks, LANES), 1)
    rank = jnp.zeros((chunks, LANES), jnp.float32)
    pos = jnp.zeros((chunks, LANES), jnp.float32)
    start = jnp.zeros((chunks, LANES), jnp.float32)
    meta = jnp.zeros((chunks, LANES), jnp.int32)
    for o in range(devices):
        member = own == o
        m16 = member.astype(jnp.float32).astype(jnp.bfloat16)
        incl = jnp.dot(m16, upper, preferred_element_type=jnp.float32) - 1.0
        total = jnp.dot(m16, ones, preferred_element_type=jnp.float32)
        off = jnp.dot(before, total.astype(jnp.bfloat16), preferred_element_type=jnp.float32)
        rank = jnp.where(member, incl + off, rank)
        pos = jnp.where(member, incl + start, pos)
        meta = jnp.where(lane == o, off.astype(jnp.int32), meta)
        turn = (off - start).astype(jnp.int32) & (LANES - 1)
        meta = jnp.where(lane == devices + o, turn, meta)
        start = start + total
        last = (off + total)[chunks - 1 : chunks, :]
        out_ref[o, 4 * tiles : 4 * tiles + 8, :] = jnp.broadcast_to(last, (8, LANES))
    rank_ref[...] = rank.astype(jnp.int32)
    pos_ref[...] = pos.astype(jnp.int32)
    meta_ref[...] = meta
    copy = pltpu.make_async_copy(meta_ref, meta_s, sem)
    copy.start()

    def sort_chunk(c):
        hot = (iota((LANES, LANES), 0) == pos_ref[pl.ds(c, 1), :]).astype(jnp.float32).astype(jnp.bfloat16)
        items = iota((8, LANES), 1).astype(jnp.float32).astype(jnp.bfloat16)
        inverse = lax.dot_general(
            items, hot, (((1,), (1,)), ((), ())), preferred_element_type=jnp.float32
        ).astype(jnp.int32)
        data_ref[c] = jnp.take_along_axis(data_ref[c], inverse, axis=1, mode="promise_in_bounds")

    for c in range(chunks):
        sort_chunk(c)
    copy.wait()
    sub8 = iota((8, LANES), 0)
    lane8 = iota((8, LANES), 1)

    def place_chunk(c, carry):
        row = data_ref[c]

        def place(o):
            off = meta_s[c, o]
            where_to = pl.ds(4 * (off >> 7), 8)
            turned = pltpu.roll(row, meta_s[c, devices + o], 1)
            keep = (sub8 < 4) & (lane8 < (off & (LANES - 1)))
            out_ref[o, where_to, :] = jnp.where(keep, out_ref[o, where_to, :], turned)

        each(devices, place, 8)
        return carry

    counts = [out_ref[o, 4 * tiles : 4 * tiles + 8, :] for o in range(devices)] if devices <= 8 else None
    if counts is None:
        last_off = meta_ref
    lax.fori_loop(0, chunks, place_chunk, 0)
    for o in range(devices):
        if counts is not None:
            out_ref[o, 4 * tiles : 4 * tiles + 8, :] = counts[o]
        else:
            n = meta_s[chunks - 1, o] + jnp.sum((own_ref[chunks - 1 : chunks, :] == o).astype(jnp.int32))
            out_ref[o, 4 * tiles : 4 * tiles + 8, :] = jnp.full((8, LANES), n, jnp.int32).astype(jnp.float32)


def lookup_kernel(
    devices, tiles, field_ref, in_ref, out_ref, table, index_v, index_s, rows_ref, sem
):
    span = tiles + 1
    for s in range(devices):
        codes = in_ref[s, pl.ds(0, span, stride=4), :].astype(jnp.int32)
        is_count = iota((span, LANES), 0) == tiles
        index_v[pl.ds(s * span, span), :] = jnp.where(is_count, codes, codes >> 6)
    copy = pltpu.make_async_copy(index_v, index_s, sem)
    copy.start()

    def build(g, carry):
        block = field_ref[pl.ds(pl.multiple_of(g * 16, 16), 16), :].astype(jnp.float32)
        for x in range(7):
            table[pl.ds(g * 128 + x, 16, stride=8), :] = block[:, 64 * x : 64 * x + 128]
        return carry

    lax.fori_loop(0, field_ref.shape[0] // 16, build, 0)
    copy.wait()
    sub8 = iota((8, LANES), 0)

    def source(s):
        count = index_s[s * span + tiles, 0]

        def tile(t, carry):
            line = s * span + t
            for p in range(LANES):
                rows_ref[p : p + 1, :] = table[pl.ds(index_s[line, p], 1), :]
            cells = rows_ref[...].T
            query = in_ref[s, pl.ds(4 * t, 4), :]
            code = query[0:1].astype(jnp.int32)
            cy = jnp.broadcast_to((code >> 3) & 7, (8, LANES))
            cz = jnp.broadcast_to(code & 7, (8, LANES))
            fx = jnp.broadcast_to(query[1:2], (8, LANES))
            fy = jnp.broadcast_to(query[2:3], (8, LANES))
            fz = jnp.broadcast_to(query[3:4], (8, LANES))
            zero = jnp.zeros((8, LANES), jnp.float32)
            inter = [zero, zero]
            slope = [zero, zero]
            for y in range(8):
                low, high = cy == y, cy == y - 1
                weight = jnp.where(low, 1.0 - fy, jnp.where(high, fy, 0.0))
                sign = jnp.where(low, -1.0, jnp.where(high, 1.0, 0.0))
                for a in range(2):
                    v = cells[64 * a + 8 * y : 64 * a + 8 * y + 8, :]
                    inter[a] = inter[a] + weight * v
                    slope[a] = slope[a] + sign * v
            low, high = cz == sub8, cz == sub8 - 1
            weight = jnp.where(low, 1.0 - fz, jnp.where(high, fz, 0.0))
            sign = jnp.where(low, -1.0, jnp.where(high, 1.0, 0.0))
            mixed = (1.0 - fx) * inter[0] + fx * inter[1]
            parts = [
                weight * mixed,
                weight * (inter[1] - inter[0]),
                weight * ((1.0 - fx) * slope[0] + fx * slope[1]),
                sign * mixed,
            ]
            out_ref[s, pl.ds(4 * t, 4), :] = jnp.concatenate(
                [jnp.sum(q, axis=0, keepdims=True) for q in parts], axis=0
            )
            return carry

        lax.fori_loop(0, (count + LANES - 1) >> 7, tile, 0)

    lax.fori_loop(0, devices, lambda s, z: (source(s), z)[1], 0)


def combine_kernel(devices, in_ref, own_ref, rank_ref, meta_s, cost_ref, grad_ref, held):
    chunks = own_ref.shape[0]
    sub8 = iota((8, LANES), 0)
    half = (sub8 >= 4).astype(jnp.int32)

    def chunk(c, carry):
        own = jnp.broadcast_to(own_ref[pl.ds(c, 1), :], (8, LANES))
        rank = jnp.broadcast_to(rank_ref[pl.ds(c, 1), :], (8, LANES))
        lane = rank & (LANES - 1)
        which = (rank >> 7) - half
        held[c] = jnp.zeros((8, LANES), jnp.float32)

        def take(o, total):
            w = meta_s[c, o] >> 7
            picked = jnp.take_along_axis(
                in_ref[o, pl.ds(4 * w, 8), :], lane, axis=1, mode="promise_in_bounds"
            )
            return jnp.where((own == o) & (which == w), picked, total)

        total = jnp.zeros((8, LANES), jnp.float32)
        if devices <= 8:
            for o in range(devices):
                total = take(o, total)
        else:
            total = lax.fori_loop(0, devices, take, total)
        held[c] = total + pltpu.roll(total, 4, 0)
        return carry

    lax.fori_loop(0, chunks, chunk, 0)
    hinge = jnp.maximum(margin - held[:, 0, :], 0.0)
    halves = grad_ref.shape[1] // LANES
    quarter = chunks // halves
    for h in range(halves):
        here = hinge[h * quarter : (h + 1) * quarter]
        cost_ref[:, h * LANES : (h + 1) * LANES] = jnp.sum(here * here, axis=0, keepdims=True)
    for k in range(3):
        grad = -2.0 * hinge * held[:, 1 + k, :]
        grad_ref[k] = jnp.concatenate(
            [grad[h * quarter : (h + 1) * quarter] for h in range(halves)], axis=1
        ).T


def exchange(x):
    return lax.all_to_all(x, "map", split_axis=0, concat_axis=0, tiled=True)


def per_device(field_bricks, owners, bricks, corners, fraction):
    devices = lax.axis_size("map")
    trajectories_here, quarter = owners.shape
    row_count = trajectories_here * quarter
    capacity = 4 * row_count // devices
    tiles = -(-capacity // LANES)
    chunks = row_count // LANES
    lines = -(-(4 * tiles + 8) // 8) * 8
    buffer = jax.ShapeDtypeStruct((devices, lines, LANES), jnp.float32)
    flat = jax.ShapeDtypeStruct((chunks, LANES), jnp.int32)
    vm = pl.BlockSpec(memory_space=VMEM)
    sm = pl.BlockSpec(memory_space=SMEM)
    outgoing, own, rank, meta = pl.pallas_call(
        functools.partial(dispatch_kernel, devices, tiles),
        out_shape=(buffer, flat, flat, flat),
        in_specs=[vm] * 4,
        out_specs=(vm,) * 4,
        scratch_shapes=[
            VMEM((chunks, 8, LANES), jnp.float32),
            VMEM((chunks, LANES), jnp.int32),
            SMEM((chunks, LANES), jnp.int32),
            pltpu.SemaphoreType.DMA(()),
        ],
        name="dispatch",
    )(owners, bricks, corners, fraction)
    incoming = exchange(outgoing)
    span = tiles + 1
    located = pl.pallas_call(
        functools.partial(lookup_kernel, devices, tiles),
        out_shape=buffer,
        in_specs=[vm] * 2,
        out_specs=vm,
        scratch_shapes=[
            VMEM((field_bricks.shape[0] * 8, LANES), jnp.float32),
            VMEM((devices * span, LANES), jnp.int32),
            SMEM((devices * span, LANES), jnp.int32),
            VMEM((LANES, LANES), jnp.float32),
            pltpu.SemaphoreType.DMA(()),
        ],
        name="lookup",
    )(field_bricks, incoming)
    returned = exchange(located)
    cost, waypoint_grad = pl.pallas_call(
        functools.partial(combine_kernel, devices),
        out_shape=(
            jax.ShapeDtypeStruct((1, trajectories_here), jnp.float32),
            jax.ShapeDtypeStruct((3, trajectories_here, quarter), jnp.float32),
        ),
        in_specs=[vm, vm, vm, sm],
        out_specs=(vm, vm),
        scratch_shapes=[VMEM((chunks, 8, LANES), jnp.float32)],
        name="combine",
    )(returned, own, rank, meta)
    return lax.psum(cost.reshape(trajectories_here), "rep"), waypoint_grad


def solution(mesh):
    placed = (
        P("map", None),
        P("map", "rep"),
        P("map", "rep"),
        P("map", "rep"),
        P(None, "map", "rep"),
    )
    return jax.shard_map(
        per_device,
        mesh=mesh,
        in_specs=placed,
        out_specs=(P("map"), P(None, "map", "rep")),
        check_vma=False,
    )
```

```python
import functools

import jax
import jax.numpy as jnp
from jax import lax
from jax.experimental import pallas as pl
from jax.experimental.pallas import tpu as pltpu
from jax.sharding import PartitionSpec as P

margin = 0.5
LANES = 128
VMEM = pltpu.VMEM
SMEM = pltpu.SMEM


MESH = pl.DeviceIdType.MESH


def lanes_of(x):
    return jnp.concatenate(
        [x[:, h * LANES : (h + 1) * LANES] for h in range(x.shape[1] // LANES)], axis=0
    )


def iota(shape, axis):
    return lax.broadcasted_iota(jnp.int32, shape, axis)


def each(count, body, unrolled):
    if count <= unrolled:
        for i in range(count):
            body(i)
    else:
        lax.fori_loop(0, count, lambda i, z: (body(i), z)[1], 0)


def dispatch_kernel(
    devices, tiles, owners_ref, bricks_ref, corners_ref, frac_ref,
    out_ref, own_ref, rank_ref, meta_ref,
    data_ref, pos_ref, meta_s, sem,
):
    own = lanes_of(owners_ref[...])
    chunks = own.shape[0]
    bricks = bricks_ref[...]
    corners = corners_ref[...]
    cx = (corners * 1338) >> 16
    cxy = (corners * 9363) >> 16
    code = bricks * 512 + cx * 64 + (cxy - cx * 7) * 8 + (corners - cxy * 7)
    code = lanes_of(code.astype(jnp.float32))
    for k in range(2):
        data_ref[:, 4 * k, :] = code
    for f in range(3):
        part = lanes_of(frac_ref[f])
        for k in range(2):
            data_ref[:, 4 * k + 1 + f, :] = part
    own_ref[...] = own
    out_ref[...] = jnp.zeros_like(out_ref)

    upper = (iota((LANES, LANES), 0) <= iota((LANES, LANES), 1)).astype(jnp.float32).astype(jnp.bfloat16)
    ones = jnp.ones((LANES, LANES), jnp.bfloat16)
    before = (iota((chunks, chunks), 0) > iota((chunks, chunks), 1)).astype(jnp.float32).astype(jnp.bfloat16)
    lane = iota((chunks, LANES), 1)
    rank = jnp.zeros((chunks, LANES), jnp.float32)
    pos = jnp.zeros((chunks, LANES), jnp.float32)
    start = jnp.zeros((chunks, LANES), jnp.float32)
    meta = jnp.zeros((chunks, LANES), jnp.int32)
    for o in range(devices):
        member = own == o
        m16 = member.astype(jnp.float32).astype(jnp.bfloat16)
        incl = jnp.dot(m16, upper, preferred_element_type=jnp.float32) - 1.0
        total = jnp.dot(m16, ones, preferred_element_type=jnp.float32)
        off = jnp.dot(before, total.astype(jnp.bfloat16), preferred_element_type=jnp.float32)
        rank = jnp.where(member, incl + off, rank)
        pos = jnp.where(member, incl + start, pos)
        meta = jnp.where(lane == o, off.astype(jnp.int32), meta)
        turn = (off - start).astype(jnp.int32) & (LANES - 1)
        meta = jnp.where(lane == devices + o, turn, meta)
        start = start + total
        last = (off + total)[chunks - 1 : chunks, :]
        out_ref[o, 4 * tiles : 4 * tiles + 8, :] = jnp.broadcast_to(last, (8, LANES))
    rank_ref[...] = rank.astype(jnp.int32)
    pos_ref[...] = pos.astype(jnp.int32)
    meta_ref[...] = meta
    copy = pltpu.make_async_copy(meta_ref, meta_s, sem)
    copy.start()

    def sort_chunk(c):
        hot = (iota((LANES, LANES), 0) == pos_ref[pl.ds(c, 1), :]).astype(jnp.float32).astype(jnp.bfloat16)
        items = iota((8, LANES), 1).astype(jnp.float32).astype(jnp.bfloat16)
        inverse = lax.dot_general(
            items, hot, (((1,), (1,)), ((), ())), preferred_element_type=jnp.float32
        ).astype(jnp.int32)
        data_ref[c] = jnp.take_along_axis(data_ref[c], inverse, axis=1, mode="promise_in_bounds")

    for c in range(chunks):
        sort_chunk(c)
    copy.wait()
    sub8 = iota((8, LANES), 0)
    lane8 = iota((8, LANES), 1)

    def place_chunk(c, carry):
        row = data_ref[c]

        def place(o):
            off = meta_s[c, o]
            where_to = pl.ds(4 * (off >> 7), 8)
            turned = pltpu.roll(row, meta_s[c, devices + o], 1)
            keep = (sub8 < 4) & (lane8 < (off & (LANES - 1)))
            out_ref[o, where_to, :] = jnp.where(keep, out_ref[o, where_to, :], turned)

        each(devices, place, 8)
        return carry

    counts = [out_ref[o, 4 * tiles : 4 * tiles + 8, :] for o in range(devices)] if devices <= 8 else None
    if counts is None:
        last_off = meta_ref
    lax.fori_loop(0, chunks, place_chunk, 0)
    for o in range(devices):
        if counts is not None:
            out_ref[o, 4 * tiles : 4 * tiles + 8, :] = counts[o]
        else:
            n = meta_s[chunks - 1, o] + jnp.sum((own_ref[chunks - 1 : chunks, :] == o).astype(jnp.int32))
            out_ref[o, 4 * tiles : 4 * tiles + 8, :] = jnp.full((8, LANES), n, jnp.int32).astype(jnp.float32)


def lookup_kernel(
    devices, tiles, field_ref, in_ref, out_ref, table, index_v, index_s, rows_ref, sem
):
    span = tiles + 1
    for s in range(devices):
        codes = in_ref[s, pl.ds(0, span, stride=4), :].astype(jnp.int32)
        is_count = iota((span, LANES), 0) == tiles
        index_v[pl.ds(s * span, span), :] = jnp.where(is_count, codes, codes >> 6)
    copy = pltpu.make_async_copy(index_v, index_s, sem)
    copy.start()

    def build(g, carry):
        block = field_ref[pl.ds(pl.multiple_of(g * 16, 16), 16), :].astype(jnp.float32)
        for x in range(7):
            table[pl.ds(g * 128 + x, 16, stride=8), :] = block[:, 64 * x : 64 * x + 128]
        return carry

    lax.fori_loop(0, field_ref.shape[0] // 16, build, 0)
    copy.wait()
    sub8 = iota((8, LANES), 0)

    def source(s):
        count = index_s[s * span + tiles, 0]

        def tile(t, carry):
            line = s * span + t
            for p in range(LANES):
                rows_ref[p : p + 1, :] = table[pl.ds(index_s[line, p], 1), :]
            cells = rows_ref[...].T
            query = in_ref[s, pl.ds(4 * t, 4), :]
            code = query[0:1].astype(jnp.int32)
            cy = jnp.broadcast_to((code >> 3) & 7, (8, LANES))
            cz = jnp.broadcast_to(code & 7, (8, LANES))
            fx = jnp.broadcast_to(query[1:2], (8, LANES))
            fy = jnp.broadcast_to(query[2:3], (8, LANES))
            fz = jnp.broadcast_to(query[3:4], (8, LANES))
            zero = jnp.zeros((8, LANES), jnp.float32)
            inter = [zero, zero]
            slope = [zero, zero]
            for y in range(8):
                low, high = cy == y, cy == y - 1
                weight = jnp.where(low, 1.0 - fy, jnp.where(high, fy, 0.0))
                sign = jnp.where(low, -1.0, jnp.where(high, 1.0, 0.0))
                for a in range(2):
                    v = cells[64 * a + 8 * y : 64 * a + 8 * y + 8, :]
                    inter[a] = inter[a] + weight * v
                    slope[a] = slope[a] + sign * v
            low, high = cz == sub8, cz == sub8 - 1
            weight = jnp.where(low, 1.0 - fz, jnp.where(high, fz, 0.0))
            sign = jnp.where(low, -1.0, jnp.where(high, 1.0, 0.0))
            mixed = (1.0 - fx) * inter[0] + fx * inter[1]
            parts = [
                weight * mixed,
                weight * (inter[1] - inter[0]),
                weight * ((1.0 - fx) * slope[0] + fx * slope[1]),
                sign * mixed,
            ]
            out_ref[s, pl.ds(4 * t, 4), :] = jnp.concatenate(
                [jnp.sum(q, axis=0, keepdims=True) for q in parts], axis=0
            )
            return carry

        lax.fori_loop(0, (count + LANES - 1) >> 7, tile, 0)

    lax.fori_loop(0, devices, lambda s, z: (source(s), z)[1], 0)


def greet(peers):
    barrier = pltpu.get_barrier_semaphore()
    for peer in peers:
        pl.semaphore_signal(barrier, inc=1, device_id=peer, device_id_type=MESH)
    pl.semaphore_wait(barrier, len(peers))


def peer_along(axis, size, step):
    return {axis: lax.rem(lax.axis_index(axis) + step, size)}


def starts(devices, lines, src_ref, dst_of, send_sem, recv_sem):
    me = lax.axis_index("map")
    copies = []
    for k in range(1, devices):
        to = lax.rem(me + k, devices)
        copy = pltpu.make_async_remote_copy(
            src_ref=src_ref.at[to, pl.ds(0, lines)],
            dst_ref=dst_of(k),
            send_sem=send_sem.at[k],
            recv_sem=recv_sem.at[k],
            device_id={"map": to},
            device_id_type=MESH,
        )
        copy.start()
        copies.append(copy)
    own = pltpu.make_async_copy(
        src_ref.at[me, pl.ds(0, lines)], dst_of(0), recv_sem.at[0]
    )
    own.start()
    return own, copies


def exchange_kernel(devices, lines, in_ref, out_ref, send_sem, recv_sem):
    greet([peer_along("map", devices, k) for k in range(1, devices)])
    me = lax.axis_index("map")
    own, copies = starts(
        devices, lines, in_ref, lambda k: out_ref.at[me, pl.ds(0, lines)], send_sem, recv_sem
    )
    own.wait()
    for copy in copies:
        copy.wait()


def combine_kernel(
    devices, reps, lines, in_ref, own_ref, rank_ref, meta_s, cost_ref, grad_ref,
    held, costs, send_sem, recv_sem, cost_send, cost_recv, *landed,
):
    greet(
        [peer_along("map", devices, k) for k in range(1, devices)]
        + [peer_along("rep", reps, k) for k in range(1, reps)]
    )
    own_copy, copies = starts(
        devices, lines, in_ref, lambda k: landed[k].at[pl.ds(0, lines)], send_sem, recv_sem
    )
    me = lax.axis_index("map")
    chunks = own_ref.shape[0]
    sub8 = iota((8, LANES), 0)
    half = (sub8 >= 4).astype(jnp.int32)
    for k in range(devices):
        if k == 0:
            own_copy.wait()
            source = me
        else:
            copies[k - 1].wait_recv()
            source = lax.rem(me + devices - k, devices)

        def chunk(c, carry):
            owner = jnp.broadcast_to(own_ref[pl.ds(c, 1), :], (8, LANES))
            rank = jnp.broadcast_to(rank_ref[pl.ds(c, 1), :], (8, LANES))
            which = (rank >> 7) - half
            w = meta_s[c, source] >> 7
            picked = jnp.take_along_axis(
                landed[k][pl.ds(4 * w, 8), :], rank & (LANES - 1), axis=1,
                mode="promise_in_bounds",
            )
            before = held[c] if k else jnp.zeros((8, LANES), jnp.float32)
            held[c] = jnp.where((owner == source) & (which == w), picked, before)
            return carry

        lax.fori_loop(0, chunks, chunk, 0, unroll=8)
    dist = held[:, 0, :] + held[:, 4, :]
    hinge = jnp.maximum(margin - dist, 0.0)
    halves = grad_ref.shape[2] // LANES
    quarter = chunks // halves
    rep = lax.axis_index("rep")
    for h in range(halves):
        here = hinge[h * quarter : (h + 1) * quarter]
        costs[0, :, h * LANES : (h + 1) * LANES] = jnp.sum(here * here, axis=0, keepdims=True)
    for n in range(3):
        grad = -2.0 * hinge * (held[:, 1 + n, :] + held[:, 5 + n, :])
        for h in range(halves):
            grad_ref[n, :, h * LANES : (h + 1) * LANES] = grad[h * quarter : (h + 1) * quarter]
    sums = []
    for k in range(1, reps):
        copy = pltpu.make_async_remote_copy(
            src_ref=costs.at[0],
            dst_ref=costs.at[k],
            send_sem=cost_send.at[k],
            recv_sem=cost_recv.at[k],
            device_id=peer_along("rep", reps, k),
            device_id_type=MESH,
        )
        copy.start()
        sums.append(copy)
    for copy in copies:
        copy.wait_send()
    total = costs[0]
    for k, copy in enumerate(sums):
        copy.wait()
        total = total + costs[k + 1]
    cost_ref[...] = total


def per_device(field_bricks, owners, bricks, corners, fraction):
    devices = lax.axis_size("map")
    trajectories_here, quarter = owners.shape
    row_count = trajectories_here * quarter
    capacity = 4 * row_count // devices
    tiles = -(-capacity // LANES)
    chunks = row_count // LANES
    lines = -(-(4 * tiles + 8) // 8) * 8
    buffer = jax.ShapeDtypeStruct((devices, lines, LANES), jnp.float32)
    flat = jax.ShapeDtypeStruct((chunks, LANES), jnp.int32)
    vm = pl.BlockSpec(memory_space=VMEM)
    sm = pl.BlockSpec(memory_space=SMEM)
    outgoing, own, rank, meta = pl.pallas_call(
        functools.partial(dispatch_kernel, devices, tiles),
        out_shape=(buffer, flat, flat, flat),
        in_specs=[vm] * 4,
        out_specs=(vm,) * 4,
        scratch_shapes=[
            VMEM((chunks, 8, LANES), jnp.float32),
            VMEM((chunks, LANES), jnp.int32),
            SMEM((chunks, LANES), jnp.int32),
            pltpu.SemaphoreType.DMA(()),
        ],
        name="dispatch",
    )(owners.T, bricks.T, corners.T, fraction.transpose(0, 2, 1))
    span = tiles + 1
    sems = pltpu.SemaphoreType.DMA((devices,))
    incoming = pl.pallas_call(
        functools.partial(exchange_kernel, devices, 4 * span),
        out_shape=buffer,
        in_specs=[vm],
        out_specs=vm,
        scratch_shapes=[sems, sems],
        compiler_params=pltpu.CompilerParams(collective_id=0, has_side_effects=True),
        name="send_queries",
    )(outgoing)
    located = pl.pallas_call(
        functools.partial(lookup_kernel, devices, tiles),
        out_shape=buffer,
        in_specs=[vm] * 2,
        out_specs=vm,
        scratch_shapes=[
            VMEM((field_bricks.shape[0] * 8, LANES), jnp.float32),
            VMEM((devices * span, LANES), jnp.int32),
            SMEM((devices * span, LANES), jnp.int32),
            VMEM((LANES, LANES), jnp.float32),
            pltpu.SemaphoreType.DMA(()),
        ],
        name="lookup",
    )(field_bricks, incoming)
    reps = lax.axis_size("rep")
    rep_sems = pltpu.SemaphoreType.DMA((reps,))
    cost, waypoint_grad = pl.pallas_call(
        functools.partial(combine_kernel, devices, reps, 4 * tiles),
        out_shape=(
            jax.ShapeDtypeStruct((1, trajectories_here), jnp.float32),
            jax.ShapeDtypeStruct((3, quarter, trajectories_here), jnp.float32),
        ),
        in_specs=[vm, vm, vm, sm],
        out_specs=(vm, vm),
        scratch_shapes=[
            VMEM((chunks, 8, LANES), jnp.float32),
            VMEM((reps, 1, trajectories_here), jnp.float32),
            sems, sems, rep_sems, rep_sems,
        ]
        + [VMEM((lines, LANES), jnp.float32)] * devices,
        compiler_params=pltpu.CompilerParams(collective_id=1, has_side_effects=True),
        name="combine",
    )(located, own, rank, meta)
    return cost.reshape(trajectories_here), waypoint_grad.transpose(0, 2, 1)


def solution(mesh):
    placed = (
        P("map", None),
        P("map", "rep"),
        P("map", "rep"),
        P("map", "rep"),
        P(None, "map", "rep"),
    )
    return jax.shard_map(
        per_device,
        mesh=mesh,
        in_specs=placed,
        out_specs=(P("map"), P(None, "map", "rep")),
        check_vma=False,
    )
```

```python
import functools

import jax
import jax.numpy as jnp
from jax import lax
from jax.experimental import pallas as pl
from jax.experimental.pallas import tpu as pltpu
from jax.sharding import PartitionSpec as P

margin = 0.5
LANES = 128
VMEM = pltpu.VMEM
SMEM = pltpu.SMEM


MESH = pl.DeviceIdType.MESH


def lanes_of(x):
    return jnp.concatenate(
        [x[:, h * LANES : (h + 1) * LANES] for h in range(x.shape[1] // LANES)], axis=0
    )


def iota(shape, axis):
    return lax.broadcasted_iota(jnp.int32, shape, axis)


def each(count, body, unrolled):
    if count <= unrolled:
        for i in range(count):
            body(i)
    else:
        lax.fori_loop(0, count, lambda i, z: (body(i), z)[1], 0)


def dispatch_kernel(
    devices, tiles, owners_ref, bricks_ref, corners_ref, frac_ref,
    out_ref, own_ref, rank_ref, meta_ref,
    data_ref, pos_ref, meta_s, sem,
):
    own = lanes_of(owners_ref[...])
    chunks = own.shape[0]
    bricks = bricks_ref[...]
    corners = corners_ref[...]
    cx = (corners * 1338) >> 16
    cxy = (corners * 9363) >> 16
    code = bricks * 512 + cx * 64 + (cxy - cx * 7) * 8 + (corners - cxy * 7)
    code = lanes_of(code.astype(jnp.float32))
    for k in range(2):
        data_ref[:, 4 * k, :] = code
    for f in range(3):
        part = lanes_of(frac_ref[f])
        for k in range(2):
            data_ref[:, 4 * k + 1 + f, :] = part
    own_ref[...] = own
    out_ref[...] = jnp.zeros_like(out_ref)

    upper = (iota((LANES, LANES), 0) <= iota((LANES, LANES), 1)).astype(jnp.float32).astype(jnp.bfloat16)
    ones = jnp.ones((LANES, LANES), jnp.bfloat16)
    before = (iota((chunks, chunks), 0) > iota((chunks, chunks), 1)).astype(jnp.float32).astype(jnp.bfloat16)
    lane = iota((chunks, LANES), 1)
    rank = jnp.zeros((chunks, LANES), jnp.float32)
    pos = jnp.zeros((chunks, LANES), jnp.float32)
    start = jnp.zeros((chunks, LANES), jnp.float32)
    meta = jnp.zeros((chunks, LANES), jnp.int32)
    for o in range(devices):
        member = own == o
        m16 = member.astype(jnp.float32).astype(jnp.bfloat16)
        incl = jnp.dot(m16, upper, preferred_element_type=jnp.float32) - 1.0
        total = jnp.dot(m16, ones, preferred_element_type=jnp.float32)
        off = jnp.dot(before, total.astype(jnp.bfloat16), preferred_element_type=jnp.float32)
        rank = jnp.where(member, incl + off, rank)
        pos = jnp.where(member, incl + start, pos)
        meta = jnp.where(lane == o, off.astype(jnp.int32), meta)
        turn = (off - start).astype(jnp.int32) & (LANES - 1)
        meta = jnp.where(lane == devices + o, turn, meta)
        start = start + total
        last = (off + total)[chunks - 1 : chunks, :]
        out_ref[o, 4 * tiles : 4 * tiles + 8, :] = jnp.broadcast_to(last, (8, LANES))
    rank_ref[...] = rank.astype(jnp.int32)
    pos_ref[...] = pos.astype(jnp.int32)
    meta_ref[...] = meta
    copy = pltpu.make_async_copy(meta_ref, meta_s, sem)
    copy.start()

    def sort_chunk(c):
        hot = (iota((LANES, LANES), 0) == pos_ref[pl.ds(c, 1), :]).astype(jnp.float32).astype(jnp.bfloat16)
        items = iota((8, LANES), 1).astype(jnp.float32).astype(jnp.bfloat16)
        inverse = lax.dot_general(
            items, hot, (((1,), (1,)), ((), ())), preferred_element_type=jnp.float32
        ).astype(jnp.int32)
        data_ref[c] = jnp.take_along_axis(data_ref[c], inverse, axis=1, mode="promise_in_bounds")

    for c in range(chunks):
        sort_chunk(c)
    copy.wait()
    sub8 = iota((8, LANES), 0)
    lane8 = iota((8, LANES), 1)

    def place_chunk(c, carry):
        row = data_ref[c]

        def place(o):
            off = meta_s[c, o]
            where_to = pl.ds(4 * (off >> 7), 8)
            turned = pltpu.roll(row, meta_s[c, devices + o], 1)
            keep = (sub8 < 4) & (lane8 < (off & (LANES - 1)))
            out_ref[o, where_to, :] = jnp.where(keep, out_ref[o, where_to, :], turned)

        each(devices, place, 8)
        return carry

    counts = [out_ref[o, 4 * tiles : 4 * tiles + 8, :] for o in range(devices)] if devices <= 8 else None
    if counts is None:
        last_off = meta_ref
    lax.fori_loop(0, chunks, place_chunk, 0)
    for o in range(devices):
        if counts is not None:
            out_ref[o, 4 * tiles : 4 * tiles + 8, :] = counts[o]
        else:
            n = meta_s[chunks - 1, o] + jnp.sum((own_ref[chunks - 1 : chunks, :] == o).astype(jnp.int32))
            out_ref[o, 4 * tiles : 4 * tiles + 8, :] = jnp.full((8, LANES), n, jnp.int32).astype(jnp.float32)


def lookup_kernel(
    devices, tiles, table, in_ref, out_ref, index_v, index_s, rows_ref, sem
):
    span = tiles + 1
    for s in range(devices):
        codes = in_ref[s, pl.ds(0, span, stride=4), :].astype(jnp.int32)
        is_count = iota((span, LANES), 0) == tiles
        index_v[pl.ds(s * span, span), :] = jnp.where(is_count, codes, codes >> 6)
    copy = pltpu.make_async_copy(index_v, index_s, sem)
    copy.start()

    copy.wait()
    sub8 = iota((8, LANES), 0)

    def source(s):
        count = index_s[s * span + tiles, 0]

        def tile(t, carry):
            line = s * span + t
            for p in range(LANES):
                rows_ref[p : p + 1, :] = table[pl.ds(index_s[line, p], 1), :]
            cells = rows_ref[...].T
            query = in_ref[s, pl.ds(4 * t, 4), :]
            code = query[0:1].astype(jnp.int32)
            cy = jnp.broadcast_to((code >> 3) & 7, (8, LANES))
            cz = jnp.broadcast_to(code & 7, (8, LANES))
            fx = jnp.broadcast_to(query[1:2], (8, LANES))
            fy = jnp.broadcast_to(query[2:3], (8, LANES))
            fz = jnp.broadcast_to(query[3:4], (8, LANES))
            zero = jnp.zeros((8, LANES), jnp.float32)
            inter = [zero, zero]
            slope = [zero, zero]
            for y in range(8):
                low, high = cy == y, cy == y - 1
                weight = jnp.where(low, 1.0 - fy, jnp.where(high, fy, 0.0))
                sign = jnp.where(low, -1.0, jnp.where(high, 1.0, 0.0))
                for a in range(2):
                    v = cells[64 * a + 8 * y : 64 * a + 8 * y + 8, :]
                    inter[a] = inter[a] + weight * v
                    slope[a] = slope[a] + sign * v
            low, high = cz == sub8, cz == sub8 - 1
            weight = jnp.where(low, 1.0 - fz, jnp.where(high, fz, 0.0))
            sign = jnp.where(low, -1.0, jnp.where(high, 1.0, 0.0))
            mixed = (1.0 - fx) * inter[0] + fx * inter[1]
            parts = [
                weight * mixed,
                weight * (inter[1] - inter[0]),
                weight * ((1.0 - fx) * slope[0] + fx * slope[1]),
                sign * mixed,
            ]
            out_ref[s, pl.ds(4 * t, 4), :] = jnp.concatenate(
                [jnp.sum(q, axis=0, keepdims=True) for q in parts], axis=0
            )
            return carry

        lax.fori_loop(0, (count + LANES - 1) >> 7, tile, 0)

    lax.fori_loop(0, devices, lambda s, z: (source(s), z)[1], 0)


def greet(peers):
    barrier = pltpu.get_barrier_semaphore()
    for peer in peers:
        pl.semaphore_signal(barrier, inc=1, device_id=peer, device_id_type=MESH)
    pl.semaphore_wait(barrier, len(peers))


def peer_along(axis, size, step):
    return {axis: lax.rem(lax.axis_index(axis) + step, size)}


def starts(devices, lines, src_ref, dst_of, send_sem, recv_sem):
    me = lax.axis_index("map")
    copies = []
    for k in range(1, devices):
        to = lax.rem(me + k, devices)
        copy = pltpu.make_async_remote_copy(
            src_ref=src_ref.at[to, pl.ds(0, lines)],
            dst_ref=dst_of(k),
            send_sem=send_sem.at[k],
            recv_sem=recv_sem.at[k],
            device_id={"map": to},
            device_id_type=MESH,
        )
        copy.start()
        copies.append(copy)
    own = pltpu.make_async_copy(
        src_ref.at[me, pl.ds(0, lines)], dst_of(0), recv_sem.at[0]
    )
    own.start()
    return own, copies


def exchange_kernel(devices, lines, in_ref, field_ref, out_ref, table, send_sem, recv_sem):
    greet([peer_along("map", devices, k) for k in range(1, devices)])
    me = lax.axis_index("map")
    own, copies = starts(
        devices, lines, in_ref, lambda k: out_ref.at[me, pl.ds(0, lines)], send_sem, recv_sem
    )
    def build(g, carry):
        block = field_ref[pl.ds(pl.multiple_of(g * 16, 16), 16), :].astype(jnp.float32)
        for x in range(7):
            table[pl.ds(g * 128 + x, 16, stride=8), :] = block[:, 64 * x : 64 * x + 128]
        return carry

    lax.fori_loop(0, field_ref.shape[0] // 16, build, 0)
    own.wait()
    for copy in copies:
        copy.wait()


def combine_kernel(
    devices, reps, lines, in_ref, own_ref, rank_ref, meta_s, cost_ref, grad_ref,
    held, costs, send_sem, recv_sem, cost_send, cost_recv, *landed,
):
    greet(
        [peer_along("map", devices, k) for k in range(1, devices)]
        + [peer_along("rep", reps, k) for k in range(1, reps)]
    )
    own_copy, copies = starts(
        devices, lines, in_ref, lambda k: landed[k].at[pl.ds(0, lines)], send_sem, recv_sem
    )
    me = lax.axis_index("map")
    chunks = own_ref.shape[0]
    sub8 = iota((8, LANES), 0)
    half = (sub8 >= 4).astype(jnp.int32)
    for k in range(devices):
        if k == 0:
            own_copy.wait()
            source = me
        else:
            copies[k - 1].wait_recv()
            source = lax.rem(me + devices - k, devices)

        def chunk(c, carry):
            owner = jnp.broadcast_to(own_ref[pl.ds(c, 1), :], (8, LANES))
            rank = jnp.broadcast_to(rank_ref[pl.ds(c, 1), :], (8, LANES))
            which = (rank >> 7) - half
            w = meta_s[c, source] >> 7
            picked = jnp.take_along_axis(
                landed[k][pl.ds(4 * w, 8), :], rank & (LANES - 1), axis=1,
                mode="promise_in_bounds",
            )
            before = held[c] if k else jnp.zeros((8, LANES), jnp.float32)
            held[c] = jnp.where((owner == source) & (which == w), picked, before)
            return carry

        lax.fori_loop(0, chunks, chunk, 0, unroll=8)
    dist = held[:, 0, :] + held[:, 4, :]
    hinge = jnp.maximum(margin - dist, 0.0)
    halves = grad_ref.shape[2] // LANES
    quarter = chunks // halves
    rep = lax.axis_index("rep")
    for h in range(halves):
        here = hinge[h * quarter : (h + 1) * quarter]
        costs[0, :, h * LANES : (h + 1) * LANES] = jnp.sum(here * here, axis=0, keepdims=True)
    for n in range(3):
        grad = -2.0 * hinge * (held[:, 1 + n, :] + held[:, 5 + n, :])
        for h in range(halves):
            grad_ref[n, :, h * LANES : (h + 1) * LANES] = grad[h * quarter : (h + 1) * quarter]
    sums = []
    for k in range(1, reps):
        copy = pltpu.make_async_remote_copy(
            src_ref=costs.at[0],
            dst_ref=costs.at[k],
            send_sem=cost_send.at[k],
            recv_sem=cost_recv.at[k],
            device_id=peer_along("rep", reps, k),
            device_id_type=MESH,
        )
        copy.start()
        sums.append(copy)
    for copy in copies:
        copy.wait_send()
    total = costs[0]
    for k, copy in enumerate(sums):
        copy.wait()
        total = total + costs[k + 1]
    cost_ref[...] = total


def per_device(field_bricks, owners, bricks, corners, fraction):
    devices = lax.axis_size("map")
    trajectories_here, quarter = owners.shape
    row_count = trajectories_here * quarter
    capacity = 4 * row_count // devices
    tiles = -(-capacity // LANES)
    chunks = row_count // LANES
    lines = -(-(4 * tiles + 8) // 8) * 8
    buffer = jax.ShapeDtypeStruct((devices, lines, LANES), jnp.float32)
    flat = jax.ShapeDtypeStruct((chunks, LANES), jnp.int32)
    vm = pl.BlockSpec(memory_space=VMEM)
    sm = pl.BlockSpec(memory_space=SMEM)
    outgoing, own, rank, meta = pl.pallas_call(
        functools.partial(dispatch_kernel, devices, tiles),
        out_shape=(buffer, flat, flat, flat),
        in_specs=[vm] * 4,
        out_specs=(vm,) * 4,
        scratch_shapes=[
            VMEM((chunks, 8, LANES), jnp.float32),
            VMEM((chunks, LANES), jnp.int32),
            SMEM((chunks, LANES), jnp.int32),
            pltpu.SemaphoreType.DMA(()),
        ],
        compiler_params=pltpu.CompilerParams(vmem_limit_bytes=16 << 20),
        name="dispatch",
    )(owners.T, bricks.T, corners.T, fraction.transpose(0, 2, 1))
    span = tiles + 1
    sems = pltpu.SemaphoreType.DMA((devices,))
    table = VMEM((field_bricks.shape[0] * 8, LANES), jnp.float32)
    incoming, table = pl.pallas_call(
        functools.partial(exchange_kernel, devices, 4 * span),
        out_shape=(buffer, table),
        in_specs=[vm, vm],
        out_specs=(vm, vm),
        scratch_shapes=[sems, sems],
        compiler_params=pltpu.CompilerParams(collective_id=0, has_side_effects=True, vmem_limit_bytes=16 << 20),
        name="send_queries",
    )(outgoing, field_bricks)
    located = pl.pallas_call(
        functools.partial(lookup_kernel, devices, tiles),
        out_shape=buffer,
        in_specs=[vm] * 2,
        out_specs=vm,
        scratch_shapes=[
            VMEM((devices * span, LANES), jnp.int32),
            SMEM((devices * span, LANES), jnp.int32),
            VMEM((LANES, LANES), jnp.float32),
            pltpu.SemaphoreType.DMA(()),
        ],
        compiler_params=pltpu.CompilerParams(vmem_limit_bytes=16 << 20),
        name="lookup",
    )(table, incoming)
    reps = lax.axis_size("rep")
    rep_sems = pltpu.SemaphoreType.DMA((reps,))
    cost, waypoint_grad = pl.pallas_call(
        functools.partial(combine_kernel, devices, reps, 4 * tiles),
        out_shape=(
            jax.ShapeDtypeStruct((1, trajectories_here), jnp.float32),
            jax.ShapeDtypeStruct((3, quarter, trajectories_here), jnp.float32),
        ),
        in_specs=[vm, vm, vm, sm],
        out_specs=(vm, vm),
        scratch_shapes=[
            VMEM((chunks, 8, LANES), jnp.float32),
            VMEM((reps, 1, trajectories_here), jnp.float32),
            sems, sems, rep_sems, rep_sems,
        ]
        + [VMEM((lines, LANES), jnp.float32)] * devices,
        compiler_params=pltpu.CompilerParams(collective_id=1, has_side_effects=True, vmem_limit_bytes=16 << 20),
        name="combine",
    )(located, own, rank, meta)
    return cost.reshape(trajectories_here), waypoint_grad.transpose(0, 2, 1)


def solution(mesh):
    placed = (
        P("map", None),
        P("map", "rep"),
        P("map", "rep"),
        P("map", "rep"),
        P(None, "map", "rep"),
    )
    return jax.shard_map(
        per_device,
        mesh=mesh,
        in_specs=placed,
        out_specs=(P("map"), P(None, "map", "rep")),
        check_vma=False,
    )
```

```python
import functools

import jax
import jax.numpy as jnp
from jax import lax
from jax.experimental import pallas as pl
from jax.experimental.pallas import tpu as pltpu
from jax.sharding import PartitionSpec as P

margin = 0.5
LANES = 128
VMEM = pltpu.VMEM
SMEM = pltpu.SMEM


MESH = pl.DeviceIdType.MESH


def lanes_of(x):
    return jnp.concatenate(
        [x[:, h * LANES : (h + 1) * LANES] for h in range(x.shape[1] // LANES)], axis=0
    )


def iota(shape, axis):
    return lax.broadcasted_iota(jnp.int32, shape, axis)


def stay(x):
    return pltpu.with_memory_space_constraint(x, pltpu.HBM)


def each(count, body, unrolled):
    if count <= unrolled:
        for i in range(count):
            body(i)
    else:
        lax.fori_loop(0, count, lambda i, z: (body(i), z)[1], 0)


def dispatch_kernel(
    devices, tiles, owners_hbm, bricks_hbm, corners_hbm, frac_hbm,
    out_ref, own_ref, rank_ref, meta_ref,
    data_ref, pos_ref, meta_s, sem, owners_ref, bricks_ref, corners_ref, frac_ref, load_sem,
):
    loads = [
        pltpu.make_async_copy(source, target, load_sem.at[i])
        for i, (source, target) in enumerate(
            [(owners_hbm, owners_ref), (bricks_hbm, bricks_ref),
             (corners_hbm, corners_ref), (frac_hbm, frac_ref)]
        )
    ]
    for load in loads:
        load.start()
    out_ref[...] = jnp.zeros_like(out_ref)
    for load in loads:
        load.wait()
    own = lanes_of(owners_ref[...])
    chunks = own.shape[0]
    bricks = bricks_ref[...]
    corners = corners_ref[...]
    cx = (corners * 1338) >> 16
    cxy = (corners * 9363) >> 16
    code = bricks * 512 + cx * 64 + (cxy - cx * 7) * 8 + (corners - cxy * 7)
    code = lanes_of(code.astype(jnp.float32))
    for k in range(2):
        data_ref[:, 4 * k, :] = code
    for f in range(3):
        part = lanes_of(frac_ref[f])
        for k in range(2):
            data_ref[:, 4 * k + 1 + f, :] = part
    own_ref[...] = own

    upper = (iota((LANES, LANES), 0) <= iota((LANES, LANES), 1)).astype(jnp.float32).astype(jnp.bfloat16)
    ones = jnp.ones((LANES, LANES), jnp.bfloat16)
    before = (iota((chunks, chunks), 0) > iota((chunks, chunks), 1)).astype(jnp.float32).astype(jnp.bfloat16)
    lane = iota((chunks, LANES), 1)
    rank = jnp.zeros((chunks, LANES), jnp.float32)
    pos = jnp.zeros((chunks, LANES), jnp.float32)
    start = jnp.zeros((chunks, LANES), jnp.float32)
    meta = jnp.zeros((chunks, LANES), jnp.int32)
    for o in range(devices):
        member = own == o
        m16 = member.astype(jnp.float32).astype(jnp.bfloat16)
        incl = jnp.dot(m16, upper, preferred_element_type=jnp.float32) - 1.0
        total = jnp.dot(m16, ones, preferred_element_type=jnp.float32)
        off = jnp.dot(before, total.astype(jnp.bfloat16), preferred_element_type=jnp.float32)
        rank = jnp.where(member, incl + off, rank)
        pos = jnp.where(member, incl + start, pos)
        meta = jnp.where(lane == o, off.astype(jnp.int32), meta)
        turn = (off - start).astype(jnp.int32) & (LANES - 1)
        meta = jnp.where(lane == devices + o, turn, meta)
        start = start + total
        last = (off + total)[chunks - 1 : chunks, :]
        out_ref[o, 4 * tiles : 4 * tiles + 8, :] = jnp.broadcast_to(last, (8, LANES))
    rank_ref[...] = rank.astype(jnp.int32)
    pos_ref[...] = pos.astype(jnp.int32)
    meta_ref[...] = meta
    copy = pltpu.make_async_copy(meta_ref, meta_s, sem)
    copy.start()

    def sort_chunk(c):
        hot = (iota((LANES, LANES), 0) == pos_ref[pl.ds(c, 1), :]).astype(jnp.float32).astype(jnp.bfloat16)
        items = iota((8, LANES), 1).astype(jnp.float32).astype(jnp.bfloat16)
        inverse = lax.dot_general(
            items, hot, (((1,), (1,)), ((), ())), preferred_element_type=jnp.float32
        ).astype(jnp.int32)
        data_ref[c] = jnp.take_along_axis(data_ref[c], inverse, axis=1, mode="promise_in_bounds")

    for c in range(chunks):
        sort_chunk(c)
    copy.wait()
    sub8 = iota((8, LANES), 0)
    lane8 = iota((8, LANES), 1)

    def place_chunk(c, carry):
        row = data_ref[c]

        def place(o):
            off = meta_s[c, o]
            where_to = pl.ds(4 * (off >> 7), 8)
            turned = pltpu.roll(row, meta_s[c, devices + o], 1)
            keep = (sub8 < 4) & (lane8 < (off & (LANES - 1)))
            out_ref[o, where_to, :] = jnp.where(keep, out_ref[o, where_to, :], turned)

        each(devices, place, 8)
        return carry

    counts = [out_ref[o, 4 * tiles : 4 * tiles + 8, :] for o in range(devices)] if devices <= 8 else None
    if counts is None:
        last_off = meta_ref
    lax.fori_loop(0, chunks, place_chunk, 0)
    for o in range(devices):
        if counts is not None:
            out_ref[o, 4 * tiles : 4 * tiles + 8, :] = counts[o]
        else:
            n = meta_s[chunks - 1, o] + jnp.sum((own_ref[chunks - 1 : chunks, :] == o).astype(jnp.int32))
            out_ref[o, 4 * tiles : 4 * tiles + 8, :] = jnp.full((8, LANES), n, jnp.int32).astype(jnp.float32)


def lookup_kernel(
    devices, tiles, table, in_ref, out_ref, index_v, index_s, rows_ref, sem
):
    span = tiles + 1
    for s in range(devices):
        codes = in_ref[s, pl.ds(0, span, stride=4), :].astype(jnp.int32)
        is_count = iota((span, LANES), 0) == tiles
        index_v[pl.ds(s * span, span), :] = jnp.where(is_count, codes, codes >> 6)
    copy = pltpu.make_async_copy(index_v, index_s, sem)
    copy.start()

    copy.wait()
    sub8 = iota((8, LANES), 0)

    def source(s):
        count = index_s[s * span + tiles, 0]

        def tile(t, carry):
            line = s * span + t
            for p in range(LANES):
                rows_ref[p : p + 1, :] = table[pl.ds(index_s[line, p], 1), :]
            cells = rows_ref[...].T
            query = in_ref[s, pl.ds(4 * t, 4), :]
            code = query[0:1].astype(jnp.int32)
            cy = jnp.broadcast_to((code >> 3) & 7, (8, LANES))
            cz = jnp.broadcast_to(code & 7, (8, LANES))
            fx = jnp.broadcast_to(query[1:2], (8, LANES))
            fy = jnp.broadcast_to(query[2:3], (8, LANES))
            fz = jnp.broadcast_to(query[3:4], (8, LANES))
            zero = jnp.zeros((8, LANES), jnp.float32)
            inter = [zero, zero]
            slope = [zero, zero]
            for y in range(8):
                low, high = cy == y, cy == y - 1
                weight = jnp.where(low, 1.0 - fy, jnp.where(high, fy, 0.0))
                sign = jnp.where(low, -1.0, jnp.where(high, 1.0, 0.0))
                for a in range(2):
                    v = cells[64 * a + 8 * y : 64 * a + 8 * y + 8, :]
                    inter[a] = inter[a] + weight * v
                    slope[a] = slope[a] + sign * v
            low, high = cz == sub8, cz == sub8 - 1
            weight = jnp.where(low, 1.0 - fz, jnp.where(high, fz, 0.0))
            sign = jnp.where(low, -1.0, jnp.where(high, 1.0, 0.0))
            mixed = (1.0 - fx) * inter[0] + fx * inter[1]
            parts = [
                weight * mixed,
                weight * (inter[1] - inter[0]),
                weight * ((1.0 - fx) * slope[0] + fx * slope[1]),
                sign * mixed,
            ]
            out_ref[s, pl.ds(4 * t, 4), :] = jnp.concatenate(
                [jnp.sum(q, axis=0, keepdims=True) for q in parts], axis=0
            )
            return carry

        lax.fori_loop(0, (count + LANES - 1) >> 7, tile, 0)

    lax.fori_loop(0, devices, lambda s, z: (source(s), z)[1], 0)


def greet(peers):
    barrier = pltpu.get_barrier_semaphore()
    for peer in peers:
        pl.semaphore_signal(barrier, inc=1, device_id=peer, device_id_type=MESH)
    pl.semaphore_wait(barrier, len(peers))


def peer_along(axis, size, step):
    return {axis: lax.rem(lax.axis_index(axis) + step, size)}


def starts(devices, lines, src_ref, dst_of, send_sem, recv_sem):
    me = lax.axis_index("map")
    copies = []
    for k in range(1, devices):
        to = lax.rem(me + k, devices)
        copy = pltpu.make_async_remote_copy(
            src_ref=src_ref.at[to, pl.ds(0, lines)],
            dst_ref=dst_of(k),
            send_sem=send_sem.at[k],
            recv_sem=recv_sem.at[k],
            device_id={"map": to},
            device_id_type=MESH,
        )
        copy.start()
        copies.append(copy)
    own = pltpu.make_async_copy(
        src_ref.at[me, pl.ds(0, lines)], dst_of(0), recv_sem.at[0]
    )
    own.start()
    return own, copies


def exchange_kernel(devices, lines, in_ref, field_hbm, out_ref, table, send_sem, recv_sem, field_ref, field_sem):
    load = pltpu.make_async_copy(field_hbm, field_ref, field_sem)
    load.start()
    greet([peer_along("map", devices, k) for k in range(1, devices)])
    me = lax.axis_index("map")
    own, copies = starts(
        devices, lines, in_ref, lambda k: out_ref.at[me, pl.ds(0, lines)], send_sem, recv_sem
    )
    def build(g, carry):
        block = field_ref[pl.ds(pl.multiple_of(g * 16, 16), 16), :].astype(jnp.float32)
        for x in range(7):
            table[pl.ds(g * 128 + x, 16, stride=8), :] = block[:, 64 * x : 64 * x + 128]
        return carry

    load.wait()
    lax.fori_loop(0, field_ref.shape[0] // 16, build, 0)
    own.wait()
    for copy in copies:
        copy.wait()


def combine_kernel(
    devices, reps, lines, in_ref, own_ref, rank_ref, meta_s, cost_ref, grad_ref,
    held, costs, send_sem, recv_sem, cost_send, cost_recv, *landed,
):
    greet(
        [peer_along("map", devices, k) for k in range(1, devices)]
        + [peer_along("rep", reps, k) for k in range(1, reps)]
    )
    own_copy, copies = starts(
        devices, lines, in_ref, lambda k: landed[k].at[pl.ds(0, lines)], send_sem, recv_sem
    )
    me = lax.axis_index("map")
    chunks = own_ref.shape[0]
    sub8 = iota((8, LANES), 0)
    half = (sub8 >= 4).astype(jnp.int32)
    for k in range(devices):
        if k == 0:
            own_copy.wait()
            source = me
        else:
            copies[k - 1].wait_recv()
            source = lax.rem(me + devices - k, devices)

        def chunk(c, carry):
            owner = jnp.broadcast_to(own_ref[pl.ds(c, 1), :], (8, LANES))
            rank = jnp.broadcast_to(rank_ref[pl.ds(c, 1), :], (8, LANES))
            which = (rank >> 7) - half
            w = meta_s[c, source] >> 7
            picked = jnp.take_along_axis(
                landed[k][pl.ds(4 * w, 8), :], rank & (LANES - 1), axis=1,
                mode="promise_in_bounds",
            )
            before = held[c] if k else jnp.zeros((8, LANES), jnp.float32)
            held[c] = jnp.where((owner == source) & (which == w), picked, before)
            return carry

        lax.fori_loop(0, chunks, chunk, 0, unroll=8)
    dist = held[:, 0, :] + held[:, 4, :]
    hinge = jnp.maximum(margin - dist, 0.0)
    halves = grad_ref.shape[2] // LANES
    quarter = chunks // halves
    rep = lax.axis_index("rep")
    for h in range(halves):
        here = hinge[h * quarter : (h + 1) * quarter]
        costs[0, :, h * LANES : (h + 1) * LANES] = jnp.sum(here * here, axis=0, keepdims=True)
    for n in range(3):
        grad = -2.0 * hinge * (held[:, 1 + n, :] + held[:, 5 + n, :])
        for h in range(halves):
            grad_ref[n, :, h * LANES : (h + 1) * LANES] = grad[h * quarter : (h + 1) * quarter]
    sums = []
    for k in range(1, reps):
        copy = pltpu.make_async_remote_copy(
            src_ref=costs.at[0],
            dst_ref=costs.at[k],
            send_sem=cost_send.at[k],
            recv_sem=cost_recv.at[k],
            device_id=peer_along("rep", reps, k),
            device_id_type=MESH,
        )
        copy.start()
        sums.append(copy)
    for copy in copies:
        copy.wait_send()
    total = costs[0]
    for k, copy in enumerate(sums):
        copy.wait()
        total = total + costs[k + 1]
    cost_ref[...] = total


def per_device(field_bricks, owners, bricks, corners, fraction):
    devices = lax.axis_size("map")
    trajectories_here, quarter = owners.shape
    row_count = trajectories_here * quarter
    capacity = 4 * row_count // devices
    tiles = -(-capacity // LANES)
    chunks = row_count // LANES
    lines = -(-(4 * tiles + 8) // 8) * 8
    buffer = jax.ShapeDtypeStruct((devices, lines, LANES), jnp.float32)
    flat = jax.ShapeDtypeStruct((chunks, LANES), jnp.int32)
    vm = pl.BlockSpec(memory_space=VMEM)
    sm = pl.BlockSpec(memory_space=SMEM)
    hbm = pl.BlockSpec(memory_space=pltpu.HBM)
    whole = VMEM((quarter, trajectories_here), jnp.int32)
    outgoing, own, rank, meta = pl.pallas_call(
        functools.partial(dispatch_kernel, devices, tiles),
        out_shape=(buffer, flat, flat, flat),
        in_specs=[hbm] * 4,
        out_specs=(vm,) * 4,
        scratch_shapes=[
            VMEM((chunks, 8, LANES), jnp.float32),
            VMEM((chunks, LANES), jnp.int32),
            SMEM((chunks, LANES), jnp.int32),
            pltpu.SemaphoreType.DMA(()),
            whole, whole, whole,
            VMEM((3, quarter, trajectories_here), jnp.float32),
            pltpu.SemaphoreType.DMA((4,)),
        ],
        compiler_params=pltpu.CompilerParams(vmem_limit_bytes=16 << 20),
        name="dispatch",
    )(*(stay(x) for x in (owners.T, bricks.T, corners.T, fraction.transpose(0, 2, 1))))
    span = tiles + 1
    sems = pltpu.SemaphoreType.DMA((devices,))
    table = VMEM((field_bricks.shape[0] * 8, LANES), jnp.float32)
    incoming, table = pl.pallas_call(
        functools.partial(exchange_kernel, devices, 4 * span),
        out_shape=(buffer, table),
        in_specs=[vm, hbm],
        out_specs=(vm, vm),
        scratch_shapes=[
            sems, sems, VMEM(field_bricks.shape, field_bricks.dtype), pltpu.SemaphoreType.DMA(()),
        ],
        compiler_params=pltpu.CompilerParams(collective_id=0, has_side_effects=True, vmem_limit_bytes=16 << 20),
        name="send_queries",
    )(outgoing, stay(field_bricks))
    located = pl.pallas_call(
        functools.partial(lookup_kernel, devices, tiles),
        out_shape=buffer,
        in_specs=[vm] * 2,
        out_specs=vm,
        scratch_shapes=[
            VMEM((devices * span, LANES), jnp.int32),
            SMEM((devices * span, LANES), jnp.int32),
            VMEM((LANES, LANES), jnp.float32),
            pltpu.SemaphoreType.DMA(()),
        ],
        compiler_params=pltpu.CompilerParams(vmem_limit_bytes=16 << 20),
        name="lookup",
    )(table, incoming)
    reps = lax.axis_size("rep")
    rep_sems = pltpu.SemaphoreType.DMA((reps,))
    cost, waypoint_grad = pl.pallas_call(
        functools.partial(combine_kernel, devices, reps, 4 * tiles),
        out_shape=(
            jax.ShapeDtypeStruct((1, trajectories_here), jnp.float32),
            jax.ShapeDtypeStruct((3, quarter, trajectories_here), jnp.float32),
        ),
        in_specs=[vm, vm, vm, sm],
        out_specs=(vm, vm),
        scratch_shapes=[
            VMEM((chunks, 8, LANES), jnp.float32),
            VMEM((reps, 1, trajectories_here), jnp.float32),
            sems, sems, rep_sems, rep_sems,
        ]
        + [VMEM((lines, LANES), jnp.float32)] * devices,
        compiler_params=pltpu.CompilerParams(collective_id=1, has_side_effects=True, vmem_limit_bytes=16 << 20),
        name="combine",
    )(located, own, rank, meta)
    return cost.reshape(trajectories_here), waypoint_grad.transpose(0, 2, 1)


def solution(mesh):
    placed = (
        P("map", None),
        P("map", "rep"),
        P("map", "rep"),
        P("map", "rep"),
        P(None, "map", "rep"),
    )
    return jax.shard_map(
        per_device,
        mesh=mesh,
        in_specs=placed,
        out_specs=(P("map"), P(None, "map", "rep")),
        check_vma=False,
    )
```
